32 devices in a mesh: grp: 16 (over z, x, core), fsdp: 2 (over y).
Axes of the slice: x: 2, y: 2, z: 4, core: 2. Of those that a mesh axis runs over, the one named last changes fastest.
Arguments:
- normalized_inputs: bfloat16 [4096, 2048], P(('grp', 'fsdp')), may hold values from -6 to 6
- output_sensitivity: bfloat16 [4096, 512], P(('grp', 'fsdp')), may hold values from -6 to 6
- projection_weights: bfloat16 [2048, 512], P('fsdp'), may hold values from -0.25 to 0.25
- completion_mask: int32 [16], replicated, may hold values 0 or 1
- replica_partition_list: int32 [16], replicated, may hold values from 0 to 3, as said below
Outputs:
- input_grad: bfloat16 [4096, 2048], P(('grp', 'fsdp'))
- weight_grad: float32 [2048, 512], P(('grp', 'fsdp'))
The draws below stay inside these ranges and needn't reach their ends.
Inputs may be any that keep to these rules, and one draw needn't show every extreme that they name: `replica_partition_list`: each of the 4 block numbers is named by exactly 4 groups.
All inputs are finite; a program needn't handle non-finite values.
Results may differ from the reference program's by a relative error of at most 0.001.
Values may be sent and summed in bfloat16 or wider, within the bound.
A program may use at most 64 MiB of HBM per device.

```python
import jax
import jax.numpy as jnp
from jax import lax

D = 2048
KVW = 512
REP = 4
REPLICA_SETS = 16
TOKENS = 4096


def draw_replica_partition_list(key, part):
    return (jax.random.permutation(key, REPLICA_SETS) // REP).astype(jnp.int32)


def plant(values, rng, smallest, largest):
    shape = values.shape
    spot = [jax.random.randint(jax.random.fold_in(rng, axis), (), 0, shape[axis]) for axis in range(len(shape))]
    values = values.at[tuple(spot)].set(smallest)
    longest = shape.index(max(shape))
    spot[longest] = (spot[longest] + 1) % shape[longest]
    return values.at[tuple(spot)].set(largest)


def raised(drawn, stream_key, source, target, parts, factor):
    owner, partner = [(jnp.arange(drawn.shape[dim]) // (drawn.shape[dim] // parts)).reshape([-1 if axis == dim else 1 for axis in range(drawn.ndim)]) for dim in (source, target)]
    chosen = jax.random.permutation(stream_key, parts)[partner]
    strong = (owner == chosen) | (owner == (partner + parts // 2) % parts)
    return jnp.where(strong, factor * drawn, drawn)


def block_scale(key, extent, pieces, low, top_value):
    level, own = 1.0, jax.random.fold_in(key, 6)
    for dim, blocks in pieces:
        steps = jnp.exp(jax.random.uniform(jax.random.fold_in(own, dim), (blocks,), jnp.float32, low / len(pieces), top_value / len(pieces)))
        level = level * jnp.repeat(steps, extent[dim] // blocks).reshape([-1 if axis == dim else 1 for axis in range(len(extent))])
    return level


def noise(rng, dims, width, reach, cuts=(), dtype=jnp.bfloat16):
    values = width * jax.random.normal(rng, dims, jnp.float32)
    if cuts:
        values = values * block_scale(rng, dims, cuts, -0.22, 0.18)
    return jnp.clip(values, -reach, reach).astype(dtype)


def gaussian_with(stream_key, extent, spread, reach, cuts, heavy, held_as=jnp.bfloat16):
    result = spread * jax.random.normal(stream_key, extent, jnp.float32)
    if cuts:
        result = result * block_scale(stream_key, extent, cuts, -0.22, 0.18)
    return jnp.clip(raised(result, jax.random.fold_in(stream_key, 3), *heavy), -reach, reach).astype(held_as)


def setup_inputs(seed: int = 0) -> dict:
    seeds = jax.random.split(jax.random.key(seed), 6)
    return {
        "normalized_inputs": gaussian_with(seeds[0], (TOKENS, D), 1.0, 6.0, ((0, 32),), (0, 1, 32, 2.75)),
        "output_sensitivity": noise(seeds[1], (TOKENS, KVW), 1.0, 6.0, ((0, 32),)),
        "projection_weights": noise(seeds[2], (D, KVW), KVW ** -0.5, 0.25, ((0, 2),)),
        "completion_mask": plant((jax.random.randint(seeds[3], (REPLICA_SETS,), 0, 4) < 3).astype(jnp.int32), jax.random.fold_in(seeds[3], 1), 0, 1),
        "replica_partition_list": draw_replica_partition_list(jax.random.fold_in(seeds[5], 71), 0),
    }


def reference(normalized_inputs, output_sensitivity, projection_weights, completion_mask, replica_partition_list):
    replica_amount = completion_mask.shape[0]
    corresponding_piece = (replica_partition_list[:, None] == replica_partition_list[None, :]).astype(jnp.int32)
    finisher_tally = jnp.sum(corresponding_piece * completion_mask[None, :], axis=1).astype(jnp.int32)
    finished_indicator = completion_mask.astype(jnp.float32)
    decode_sum = finished_indicator / (finisher_tally.astype(jnp.float32) + 1.0 - finished_indicator)
    input_grad = jnp.dot(output_sensitivity, projection_weights.T, preferred_element_type=jnp.float32).astype(jnp.bfloat16)
    model_width = normalized_inputs.shape[1]
    value_width = output_sensitivity.shape[1]
    group_rows = normalized_inputs.shape[0] // replica_amount
    acts_grouped = normalized_inputs.reshape(replica_amount, group_rows, model_width)
    cots_grouped = output_sensitivity.reshape(replica_amount, group_rows, value_width)

    def accumulate(running, pieces_in):
        acts_here, cots_here, scale_here = pieces_in
        product = lax.dot_general(acts_here, cots_here, (((0,), (0,)), ((), ())), preferred_element_type=jnp.float32)
        return running + scale_here * product, None

    initial = jnp.zeros((model_width, value_width), jnp.float32)
    weight_grad, _ = lax.scan(accumulate, initial, (acts_grouped, cots_grouped, decode_sum))
    return input_grad, weight_grad
```

```python
import functools

import jax
import jax.numpy as jnp
from jax import lax
from jax.experimental import pallas as pl
from jax.experimental.pallas import tpu as pltpu
from jax.sharding import PartitionSpec as P

MESH = pl.DeviceIdType.MESH
CORES = 2
WIDE = 2


def collective_shards(
    normalized_inputs,
    output_sensitivity,
    projection_weights,
    completion_mask,
    replica_partition_list,
):
    replica_index = lax.axis_index("grp")
    selected_replica = lax.iota(jnp.int32, completion_mask.shape[0]) == replica_index
    assigned_piece = jnp.sum(jnp.where(selected_replica, replica_partition_list, 0))
    finished_indicator = jnp.sum(jnp.where(selected_replica, completion_mask, 0))
    finisher_tally = jnp.sum(
        jnp.where(replica_partition_list == assigned_piece, completion_mask, 0)
    )
    living_float = finished_indicator.astype(jnp.float32)
    decode_sum = living_float / (finisher_tally.astype(jnp.float32) + 1.0 - living_float)
    tokens_here = normalized_inputs.shape[0]
    model_width = normalized_inputs.shape[1]
    inner_size = lax.axis_size("fsdp")
    outer_size = lax.axis_size("grp")
    input_grad = lax.dot_general(
        output_sensitivity,
        lax.all_gather(projection_weights, "fsdp", axis=0, tiled=True),
        (((1,), (1,)), ((), ())),
        preferred_element_type=jnp.float32,
    ).astype(jnp.bfloat16)
    owner_rows = model_width // (outer_size * inner_size)
    reordered = normalized_inputs.reshape(tokens_here, outer_size, inner_size, owner_rows)
    reordered = reordered.transpose(0, 2, 1, 3).reshape(tokens_here, model_width)
    column_block = lax.all_to_all(reordered, "fsdp", split_axis=1, concat_axis=0, tiled=True)
    group_block = lax.dot_general(
        column_block,
        lax.all_gather(output_sensitivity, "fsdp", axis=0, tiled=True),
        (((0,), (0,)), ((), ())),
        preferred_element_type=jnp.float32,
    )
    weight_grad = lax.psum_scatter(decode_sum * group_block, "grp", scatter_dimension=0, tiled=True)
    return (input_grad, weight_grad)


def kernel(
    deep,
    mask_ref, list_ref, x_hbm, s_hbm, w_hbm,
    ig_hbm, wg_ref,
    x_v, s_v, w_v, tx, rx, px_send, px_recv, q, zr, ig_own, ig_send, ig_recv,
    load_sem, out_sem, s_send_sem, s_recv_sem, x_send_sem, x_recv_sem,
    px_send_sem, px_recv_sem, z_send_sem, z_recv_sem, ig_send_sem, ig_recv_sem,
):
    grp = lax.axis_index("grp")
    y = lax.axis_index("fsdp")
    core = lax.rem(grp, CORES)
    wide = lax.rem(grp // CORES, WIDE)
    z = grp // (CORES * WIDE)
    oy, oc = 1 - y, 1 - core
    tokens = s_hbm.shape[0]
    groups = mask_ref.shape[0]
    rows = wg_ref.shape[0]
    half = w_hbm.shape[0]

    def at(zz, xx, cc, yy):
        return ((zz * WIDE + xx) * CORES + cc, yy)

    def remote(src, dst, send, recv, device):
        copy = pltpu.make_async_remote_copy(
            src_ref=src, dst_ref=dst, send_sem=send, recv_sem=recv,
            device_id=device, device_id_type=MESH,
        )
        return copy

    y_peer = at(z, wide, core, oy)
    y_cross = at(z, wide, oc, oy)
    sibling = at(z, wide, oc, y)
    x_peer = at(z, 1 - wide, core, y)
    z_to = [at(lax.rem(z + k, deep), wide, core, y) for k in range(1, deep)]
    me = core * 2 + y
    from_y = core * 2 + oy
    from_cross = oc * 2 + oy
    from_sib = oc * 2 + y

    load_s = pltpu.make_async_copy(s_hbm, s_v.at[me], load_sem.at[0])
    load_x = pltpu.make_async_copy(x_hbm, x_v, load_sem.at[1])
    load_w = pltpu.make_async_copy(w_hbm, w_v, load_sem.at[2])
    load_s.start()
    load_x.start()
    load_w.start()

    barrier = pltpu.get_barrier_semaphore()
    partners = [y_peer, y_cross, sibling, x_peer] + z_to
    for partner in partners:
        pl.semaphore_signal(barrier, inc=1, device_id=partner, device_id_type=MESH)

    order = [k for k in range(1, deep)] + [0]
    span = WIDE * CORES * 2 * rows

    def turn(k):
        zz = lax.rem(z + k, deep)
        part = x_v[:, pl.ds(pl.multiple_of(zz * span, span), span)].T
        for xx in range(WIDE):
            for cy in range(CORES * 2):
                start = (xx * CORES * 2 + cy) * rows
                tx[k, cy, xx * rows:(xx + 1) * rows, :] = part[start:start + rows, :]

    load_x.wait()
    turn(order[0])
    load_s.wait()
    pl.semaphore_wait(barrier, len(partners))

    s_y = remote(s_v.at[me], s_v.at[me], s_send_sem.at[0], s_recv_sem.at[0], y_peer)
    s_sib = remote(s_v.at[me], s_v.at[me], s_send_sem.at[1], s_recv_sem.at[1], sibling)
    s_fwd = remote(s_v.at[from_y], s_v.at[from_y], s_send_sem.at[2], s_recv_sem.at[2], sibling)
    s_y.start()
    s_sib.start()

    x_copies = {}
    for n, k in enumerate(order):
        if n:
            turn(k)
        copies = []
        for slot, (device, there) in enumerate(
            ((y_peer, from_y), (y_cross, from_cross), (sibling, from_sib))
        ):
            copy = remote(
                tx.at[k, there], rx.at[k, me], x_send_sem.at[k, slot], x_recv_sem.at[k, slot], device
            )
            copy.start()
            copies.append(copy)
        x_copies[k] = copies
        rx[k, me] = tx[k, me]

    scales = []
    for cc in range(CORES):
        here = (z * WIDE + wide) * CORES + cc
        mine = list_ref[here]
        tally = jnp.int32(0)
        for h in range(groups):
            tally = tally + jnp.where(list_ref[h] == mine, mask_ref[h], 0)
        done = jnp.full((1, wg_ref.shape[1]), mask_ref[here], jnp.int32).astype(jnp.float32)
        total = jnp.full((1, wg_ref.shape[1]), tally, jnp.int32).astype(jnp.float32)
        scales.append(done / (total + 1.0 - done))

    load_w.wait()

    def grad(s_block):
        return lax.dot_general(
            s_block, w_v[...], (((1,), (1,)), ((), ())), preferred_element_type=jnp.float32
        ).astype(jnp.bfloat16)

    own_columns = pl.ds(pl.multiple_of(y * half, half), half)
    other_columns = pl.ds(pl.multiple_of(oy * half, half), half)
    ig_own[...] = grad(s_v[me])
    own_out = pltpu.make_async_copy(ig_own, ig_hbm.at[:, own_columns], out_sem.at[0])
    own_out.start()

    s_y.wait_recv()
    s_fwd.start()
    ig_send[...] = grad(s_v[from_y])
    ig_copy = remote(ig_send, ig_recv, ig_send_sem, ig_recv_sem, y_peer)
    ig_copy.start()

    s_sib.wait_recv()
    s_fwd.wait_recv()

    px_copies, z_copies = {}, {}

    def partial(k):
        for copy in x_copies[k]:
            copy.wait_recv()
        total = None
        for cc in range(CORES):
            left = jnp.concatenate([rx[k, cc * 2], rx[k, cc * 2 + 1]], axis=1)
            right = s_v[cc * 2:cc * 2 + 2].reshape(2 * tokens, s_v.shape[2])
            product = scales[cc] * jnp.dot(left, right, preferred_element_type=jnp.float32)
            total = product if total is None else total + product
        for xx in range(WIDE):
            q_or_send[xx](k, total[xx * rows:(xx + 1) * rows])

    def put0(k, value):
        both[k, 0] = value

    def put1(k, value):
        both[k, 1] = value

    both = px_send
    q_or_send = (put0, put1)

    def send_x(k):
        copy = remote(
            px_send.at[k, 1 - wide], px_recv.at[k], px_send_sem.at[k], px_recv_sem.at[k], x_peer
        )
        copy.start()
        px_copies[k] = copy

    def gather_x(k):
        px_copies[k].wait_recv()
        q[k] = px_send[k, wide] + px_recv[k]
        if k:
            copy = remote(q.at[k], zr.at[k], z_send_sem.at[k], z_recv_sem.at[k], z_to[k - 1])
            copy.start()
            z_copies[k] = copy

    for n, k in enumerate(order):
        partial(k)
        send_x(k)
        if n:
            gather_x(order[n - 1])
    gather_x(order[-1])

    total = q[0]
    for k in range(1, deep):
        z_copies[k].wait_recv()
        total = total + zr[k]
    wg_ref[...] = total

    ig_copy.wait_recv()
    other_out = pltpu.make_async_copy(ig_recv, ig_hbm.at[:, other_columns], out_sem.at[1])
    other_out.start()

    for copy in (s_y, s_sib, s_fwd, ig_copy):
        copy.wait_send()
    for copies in x_copies.values():
        for copy in copies:
            copy.wait_send()
    for copy in list(px_copies.values()) + list(z_copies.values()):
        copy.wait_send()
    own_out.wait()
    other_out.wait()


def kernel_shards(deep, rows, x, s, w, mask, plist):
    tokens, width = x.shape
    values = s.shape[1]
    f32, bf16 = jnp.float32, jnp.bfloat16
    dma = pltpu.SemaphoreType.DMA
    anywhere = pl.BlockSpec(memory_space=pl.ANY)
    smem = pl.BlockSpec(memory_space=pltpu.SMEM)
    wide_rows = WIDE * rows
    return pl.pallas_call(
        functools.partial(kernel, deep),
        out_shape=(
            jax.ShapeDtypeStruct((tokens, width), bf16),
            jax.ShapeDtypeStruct((rows, values), f32),
        ),
        in_specs=[smem, smem, anywhere, anywhere, anywhere],
        out_specs=(anywhere, pl.BlockSpec(memory_space=pltpu.VMEM)),
        scratch_shapes=[
            pltpu.VMEM((tokens, width), bf16),
            pltpu.VMEM((CORES * 2, tokens, values), bf16),
            pltpu.VMEM(w.shape, bf16),
            pltpu.VMEM((deep, CORES * 2, wide_rows, tokens), bf16),
            pltpu.VMEM((deep, CORES * 2, wide_rows, tokens), bf16),
            pltpu.VMEM((deep, WIDE, rows, values), f32),
            pltpu.VMEM((deep, rows, values), f32),
            pltpu.VMEM((deep, rows, values), f32),
            pltpu.VMEM((deep, rows, values), f32),
            pltpu.VMEM((tokens, w.shape[0]), bf16),
            pltpu.VMEM((tokens, w.shape[0]), bf16),
            pltpu.VMEM((tokens, w.shape[0]), bf16),
            dma((3,)), dma((2,)), dma((3,)), dma((3,)), dma((deep, 3)), dma((deep, 3)),
            dma((deep,)), dma((deep,)), dma((deep,)), dma((deep,)), dma, dma,
        ],
        compiler_params=pltpu.CompilerParams(collective_id=0, has_side_effects=True),
    )(mask, plist, x, s, w)


def solution(mesh):
    outer, inner = mesh.shape["grp"], mesh.shape["fsdp"]

    def shards(x, s, w, mask, plist):
        rows = x.shape[1] // (outer * inner)
        if inner == 2 and outer % (CORES * WIDE) == 0 and rows % 16 == 0 and x.shape[0] % 128 == 0:
            return tuple(kernel_shards(outer // (CORES * WIDE), rows, x, s, w, mask, plist))
        return collective_shards(x, s, w, mask, plist)

    in_specs = (P(("grp", "fsdp"), None), P(("grp", "fsdp"), None), P("fsdp", None), P(), P())
    out_specs = (P(("grp", "fsdp"), None), P(("grp", "fsdp"), None))
    return jax.shard_map(shards, mesh=mesh, in_specs=in_specs, out_specs=out_specs, check_vma=False)
```

```python
import functools

import jax
import jax.numpy as jnp
from jax import lax
from jax.experimental import pallas as pl
from jax.experimental.pallas import tpu as pltpu
from jax.sharding import PartitionSpec as P

MESH = pl.DeviceIdType.MESH
CORES = 2
WIDE = 2
STEPS = 32766.0
TINY = 1e-33


def collective_shards(
    normalized_inputs,
    output_sensitivity,
    projection_weights,
    completion_mask,
    replica_partition_list,
):
    replica_index = lax.axis_index("grp")
    selected_replica = lax.iota(jnp.int32, completion_mask.shape[0]) == replica_index
    assigned_piece = jnp.sum(jnp.where(selected_replica, replica_partition_list, 0))
    finished_indicator = jnp.sum(jnp.where(selected_replica, completion_mask, 0))
    finisher_tally = jnp.sum(
        jnp.where(replica_partition_list == assigned_piece, completion_mask, 0)
    )
    living_float = finished_indicator.astype(jnp.float32)
    decode_sum = living_float / (finisher_tally.astype(jnp.float32) + 1.0 - living_float)
    tokens_here = normalized_inputs.shape[0]
    model_width = normalized_inputs.shape[1]
    inner_size = lax.axis_size("fsdp")
    outer_size = lax.axis_size("grp")
    input_grad = lax.dot_general(
        output_sensitivity,
        lax.all_gather(projection_weights, "fsdp", axis=0, tiled=True),
        (((1,), (1,)), ((), ())),
        preferred_element_type=jnp.float32,
    ).astype(jnp.bfloat16)
    owner_rows = model_width // (outer_size * inner_size)
    reordered = normalized_inputs.reshape(tokens_here, outer_size, inner_size, owner_rows)
    reordered = reordered.transpose(0, 2, 1, 3).reshape(tokens_here, model_width)
    column_block = lax.all_to_all(reordered, "fsdp", split_axis=1, concat_axis=0, tiled=True)
    group_block = lax.dot_general(
        column_block,
        lax.all_gather(output_sensitivity, "fsdp", axis=0, tiled=True),
        (((0,), (0,)), ((), ())),
        preferred_element_type=jnp.float32,
    )
    weight_grad = lax.psum_scatter(decode_sum * group_block, "grp", scatter_dimension=0, tiled=True)
    return (input_grad, weight_grad)


def encode(value):
    top = jnp.maximum(jnp.max(jnp.abs(value), axis=0, keepdims=True), TINY)
    coded = jnp.round(value * (STEPS / top)).astype(jnp.int32).astype(jnp.int16)
    return coded, top * (1.0 / STEPS)


def decoded(coded, step):
    return coded.astype(jnp.int32).astype(jnp.float32) * step


def kernel(
    deep,
    mask_ref, list_ref, x_hbm, s_hbm, w_hbm,
    ig_hbm, wg_ref,
    x_v, s_v, w_v, tx, rx, own_part, px_send, px_scale, px_recv, px_rscale,
    q, q_send, q_scale, zr, zr_scale, ig_own, ig_send, ig_recv,
    load_sem, out_sem, s_send_sem, s_recv_sem, x_send_sem, x_recv_sem,
    px_send_sem, px_recv_sem, z_send_sem, z_recv_sem, ig_send_sem, ig_recv_sem,
):
    grp = lax.axis_index("grp")
    y = lax.axis_index("fsdp")
    core = lax.rem(grp, CORES)
    wide = lax.rem(grp // CORES, WIDE)
    z = grp // (CORES * WIDE)
    oy, oc = 1 - y, 1 - core
    tokens = s_hbm.shape[0]
    groups = mask_ref.shape[0]
    rows = wg_ref.shape[0]
    half = w_hbm.shape[0]

    def at(zz, xx, cc, yy):
        return ((zz * WIDE + xx) * CORES + cc, yy)

    def remote(src, dst, send, recv, device):
        copy = pltpu.make_async_remote_copy(
            src_ref=src, dst_ref=dst, send_sem=send, recv_sem=recv,
            device_id=device, device_id_type=MESH,
        )
        return copy

    y_peer = at(z, wide, core, oy)
    y_cross = at(z, wide, oc, oy)
    sibling = at(z, wide, oc, y)
    x_peer = at(z, 1 - wide, core, y)
    z_to = [at(lax.rem(z + k, deep), wide, core, y) for k in range(1, deep)]
    me = core * 2 + y
    from_y = core * 2 + oy
    from_cross = oc * 2 + oy
    from_sib = oc * 2 + y

    load_s = pltpu.make_async_copy(s_hbm, s_v.at[me], load_sem.at[0])
    load_x = pltpu.make_async_copy(x_hbm, x_v, load_sem.at[1])
    load_w = pltpu.make_async_copy(w_hbm, w_v, load_sem.at[2])
    load_s.start()
    load_x.start()
    load_w.start()

    barrier = pltpu.get_barrier_semaphore()
    partners = [y_peer, y_cross, sibling, x_peer] + z_to
    for partner in partners:
        pl.semaphore_signal(barrier, inc=1, device_id=partner, device_id_type=MESH)

    order = [k for k in range(1, deep)] + [0]
    span = WIDE * CORES * 2 * rows

    def turn(k):
        zz = lax.rem(z + k, deep)
        part = x_v[:, pl.ds(pl.multiple_of(zz * span, span), span)].T
        for xx in range(WIDE):
            for cy in range(CORES * 2):
                start = (xx * CORES * 2 + cy) * rows
                tx[k, cy, xx * rows:(xx + 1) * rows, :] = part[start:start + rows, :]

    load_x.wait()
    turn(order[0])
    load_s.wait()
    pl.semaphore_wait(barrier, len(partners))

    s_y = remote(s_v.at[me], s_v.at[me], s_send_sem.at[0], s_recv_sem.at[0], y_peer)
    s_sib = remote(s_v.at[me], s_v.at[me], s_send_sem.at[1], s_recv_sem.at[1], sibling)
    s_fwd = remote(s_v.at[from_y], s_v.at[from_y], s_send_sem.at[2], s_recv_sem.at[2], sibling)
    s_y.start()
    s_sib.start()

    x_copies = {}
    for n, k in enumerate(order):
        if n:
            turn(k)
        copies = []
        for slot, (device, there) in enumerate(
            ((y_peer, from_y), (y_cross, from_cross), (sibling, from_sib))
        ):
            copy = remote(
                tx.at[k, there], rx.at[k, me], x_send_sem.at[k, slot], x_recv_sem.at[k, slot], device
            )
            copy.start()
            copies.append(copy)
        x_copies[k] = copies
        rx[k, me] = tx[k, me]

    scales = []
    for cc in range(CORES):
        here = (z * WIDE + wide) * CORES + cc
        mine = list_ref[here]
        tally = jnp.int32(0)
        for h in range(groups):
            tally = tally + jnp.where(list_ref[h] == mine, mask_ref[h], 0)
        done = jnp.full((1, wg_ref.shape[1]), mask_ref[here], jnp.int32).astype(jnp.float32)
        total = jnp.full((1, wg_ref.shape[1]), tally, jnp.int32).astype(jnp.float32)
        scales.append(done / (total + 1.0 - done))

    load_w.wait()

    def grad(s_block):
        return lax.dot_general(
            s_block, w_v[...], (((1,), (1,)), ((), ())), preferred_element_type=jnp.float32
        ).astype(jnp.bfloat16)

    own_columns = pl.ds(pl.multiple_of(y * half, half), half)
    other_columns = pl.ds(pl.multiple_of(oy * half, half), half)
    ig_own[...] = grad(s_v[me])
    own_out = pltpu.make_async_copy(ig_own, ig_hbm.at[:, own_columns], out_sem.at[0])
    own_out.start()

    s_y.wait_recv()
    s_fwd.start()
    ig_send[...] = grad(s_v[from_y])
    ig_copy = remote(ig_send, ig_recv, ig_send_sem, ig_recv_sem, y_peer)
    ig_copy.start()

    s_sib.wait_recv()
    s_fwd.wait_recv()

    px_copies, z_copies = {}, {}

    def partial(k):
        for copy in x_copies[k]:
            copy.wait_recv()
        total = None
        for cc in range(CORES):
            left = jnp.concatenate([rx[k, cc * 2], rx[k, cc * 2 + 1]], axis=1)
            right = s_v[cc * 2:cc * 2 + 2].reshape(2 * tokens, s_v.shape[2])
            product = scales[cc] * jnp.dot(left, right, preferred_element_type=jnp.float32)
            total = product if total is None else total + product
        own_part[k, 0] = total[:rows]
        own_part[k, 1] = total[rows:]
        coded, scale = encode(own_part[k, 1 - wide])
        px_send[k] = coded
        px_scale[k] = scale

    def send_x(k):
        copies = [
            remote(px_send.at[k], px_recv.at[k], px_send_sem.at[k, 0], px_recv_sem.at[k, 0], x_peer),
            remote(px_scale.at[k], px_rscale.at[k], px_send_sem.at[k, 1], px_recv_sem.at[k, 1], x_peer),
        ]
        for copy in copies:
            copy.start()
        px_copies[k] = copies

    def gather_x(k):
        for copy in px_copies[k]:
            copy.wait_recv()
        value = own_part[k, wide] + decoded(px_recv[k], px_rscale[k])
        if k:
            coded, scale = encode(value)
            q_send[k] = coded
            q_scale[k] = scale
            copies = [
                remote(q_send.at[k], zr.at[k], z_send_sem.at[k, 0], z_recv_sem.at[k, 0], z_to[k - 1]),
                remote(q_scale.at[k], zr_scale.at[k], z_send_sem.at[k, 1], z_recv_sem.at[k, 1], z_to[k - 1]),
            ]
            for copy in copies:
                copy.start()
            z_copies[k] = copies
        else:
            q[...] = value

    for n, k in enumerate(order):
        partial(k)
        send_x(k)
        if n:
            gather_x(order[n - 1])
    gather_x(order[-1])

    total = q[...]
    for k in range(1, deep):
        for copy in z_copies[k]:
            copy.wait_recv()
        total = total + decoded(zr[k], zr_scale[k])
    wg_ref[...] = total

    ig_copy.wait_recv()
    other_out = pltpu.make_async_copy(ig_recv, ig_hbm.at[:, other_columns], out_sem.at[1])
    other_out.start()

    for copy in (s_y, s_sib, s_fwd, ig_copy):
        copy.wait_send()
    for group in (x_copies, px_copies, z_copies):
        for copies in group.values():
            for copy in copies:
                copy.wait_send()
    own_out.wait()
    other_out.wait()


def kernel_shards(deep, rows, x, s, w, mask, plist):
    tokens, width = x.shape
    values = s.shape[1]
    f32, bf16, i16 = jnp.float32, jnp.bfloat16, jnp.int16
    dma = pltpu.SemaphoreType.DMA
    anywhere = pl.BlockSpec(memory_space=pl.ANY)
    smem = pl.BlockSpec(memory_space=pltpu.SMEM)
    wide_rows = WIDE * rows
    return pl.pallas_call(
        functools.partial(kernel, deep),
        out_shape=(
            jax.ShapeDtypeStruct((tokens, width), bf16),
            jax.ShapeDtypeStruct((rows, values), f32),
        ),
        in_specs=[smem, smem, anywhere, anywhere, anywhere],
        out_specs=(anywhere, pl.BlockSpec(memory_space=pltpu.VMEM)),
        scratch_shapes=[
            pltpu.VMEM((tokens, width), bf16),
            pltpu.VMEM((CORES * 2, tokens, values), bf16),
            pltpu.VMEM(w.shape, bf16),
            pltpu.VMEM((deep, CORES * 2, wide_rows, tokens), bf16),
            pltpu.VMEM((deep, CORES * 2, wide_rows, tokens), bf16),
            pltpu.VMEM((deep, WIDE, rows, values), f32),
            pltpu.VMEM((deep, rows, values), i16),
            pltpu.VMEM((deep, 1, values), f32),
            pltpu.VMEM((deep, rows, values), i16),
            pltpu.VMEM((deep, 1, values), f32),
            pltpu.VMEM((rows, values), f32),
            pltpu.VMEM((deep, rows, values), i16),
            pltpu.VMEM((deep, 1, values), f32),
            pltpu.VMEM((deep, rows, values), i16),
            pltpu.VMEM((deep, 1, values), f32),
            pltpu.VMEM((tokens, w.shape[0]), bf16),
            pltpu.VMEM((tokens, w.shape[0]), bf16),
            pltpu.VMEM((tokens, w.shape[0]), bf16),
            dma((3,)), dma((2,)), dma((3,)), dma((3,)), dma((deep, 3)), dma((deep, 3)),
            dma((deep, 2)), dma((deep, 2)), dma((deep, 2)), dma((deep, 2)), dma, dma,
        ],
        compiler_params=pltpu.CompilerParams(collective_id=0, has_side_effects=True),
    )(mask, plist, x, s, w)


def solution(mesh):
    outer, inner = mesh.shape["grp"], mesh.shape["fsdp"]

    def shards(x, s, w, mask, plist):
        rows = x.shape[1] // (outer * inner)
        if inner == 2 and outer % (CORES * WIDE) == 0 and rows % 16 == 0 and x.shape[0] % 128 == 0:
            return tuple(kernel_shards(outer // (CORES * WIDE), rows, x, s, w, mask, plist))
        return collective_shards(x, s, w, mask, plist)

    in_specs = (P(("grp", "fsdp"), None), P(("grp", "fsdp"), None), P("fsdp", None), P(), P())
    out_specs = (P(("grp", "fsdp"), None), P(("grp", "fsdp"), None))
    return jax.shard_map(shards, mesh=mesh, in_specs=in_specs, out_specs=out_specs, check_vma=False)
```

```python
import functools

import jax
import jax.numpy as jnp
from jax import lax
from jax.experimental import pallas as pl
from jax.experimental.pallas import tpu as pltpu
from jax.sharding import PartitionSpec as P

MESH = pl.DeviceIdType.MESH
CORES = 2
WIDE = 2
STEPS = 32766.0
TINY = 1e-33


def collective_shards(
    normalized_inputs,
    output_sensitivity,
    projection_weights,
    completion_mask,
    replica_partition_list,
):
    replica_index = lax.axis_index("grp")
    selected_replica = lax.iota(jnp.int32, completion_mask.shape[0]) == replica_index
    assigned_piece = jnp.sum(jnp.where(selected_replica, replica_partition_list, 0))
    finished_indicator = jnp.sum(jnp.where(selected_replica, completion_mask, 0))
    finisher_tally = jnp.sum(
        jnp.where(replica_partition_list == assigned_piece, completion_mask, 0)
    )
    living_float = finished_indicator.astype(jnp.float32)
    decode_sum = living_float / (finisher_tally.astype(jnp.float32) + 1.0 - living_float)
    tokens_here = normalized_inputs.shape[0]
    model_width = normalized_inputs.shape[1]
    inner_size = lax.axis_size("fsdp")
    outer_size = lax.axis_size("grp")
    input_grad = lax.dot_general(
        output_sensitivity,
        lax.all_gather(projection_weights, "fsdp", axis=0, tiled=True),
        (((1,), (1,)), ((), ())),
        preferred_element_type=jnp.float32,
    ).astype(jnp.bfloat16)
    owner_rows = model_width // (outer_size * inner_size)
    reordered = normalized_inputs.reshape(tokens_here, outer_size, inner_size, owner_rows)
    reordered = reordered.transpose(0, 2, 1, 3).reshape(tokens_here, model_width)
    column_block = lax.all_to_all(reordered, "fsdp", split_axis=1, concat_axis=0, tiled=True)
    group_block = lax.dot_general(
        column_block,
        lax.all_gather(output_sensitivity, "fsdp", axis=0, tiled=True),
        (((0,), (0,)), ((), ())),
        preferred_element_type=jnp.float32,
    )
    weight_grad = lax.psum_scatter(decode_sum * group_block, "grp", scatter_dimension=0, tiled=True)
    return (input_grad, weight_grad)


def encode(value):
    top = jnp.maximum(jnp.max(jnp.abs(value), axis=0, keepdims=True), TINY)
    coded = jnp.round(value * (STEPS / top)).astype(jnp.int32).astype(jnp.int16)
    return coded, top * (1.0 / STEPS)


def decoded(coded, step):
    return coded.astype(jnp.int32).astype(jnp.float32) * step


def kernel(
    deep,
    mask_ref, list_ref, x_hbm, s_hbm, w_hbm,
    ig_ref, wg_ref,
    x_v, s_v, w_v, tx, rx, own_part, px_send, px_scale, px_recv, px_rscale,
    q, q_send, q_scale, zr, zr_scale, ig_send,
    load_sem, s_send_sem, s_recv_sem, x_send_sem, x_recv_sem,
    px_send_sem, px_recv_sem, z_send_sem, z_recv_sem, ig_send_sem, ig_recv_sem,
):
    grp = lax.axis_index("grp")
    y = lax.axis_index("fsdp")
    core = lax.rem(grp, CORES)
    wide = lax.rem(grp // CORES, WIDE)
    z = grp // (CORES * WIDE)
    oy, oc = 1 - y, 1 - core
    tokens = s_hbm.shape[0]
    groups = mask_ref.shape[0]
    rows = wg_ref.shape[0]
    half = w_hbm.shape[0]

    def at(zz, xx, cc, yy):
        return ((zz * WIDE + xx) * CORES + cc, yy)

    def remote(src, dst, send, recv, device):
        copy = pltpu.make_async_remote_copy(
            src_ref=src, dst_ref=dst, send_sem=send, recv_sem=recv,
            device_id=device, device_id_type=MESH,
        )
        return copy

    y_peer = at(z, wide, core, oy)
    y_cross = at(z, wide, oc, oy)
    sibling = at(z, wide, oc, y)
    x_peer = at(z, 1 - wide, core, y)
    z_to = [at(lax.rem(z + k, deep), wide, core, y) for k in range(1, deep)]
    me = core * 2 + y
    from_y = core * 2 + oy
    from_cross = oc * 2 + oy
    from_sib = oc * 2 + y

    load_s = pltpu.make_async_copy(s_hbm, s_v.at[me], load_sem.at[0])
    load_x = pltpu.make_async_copy(x_hbm, x_v, load_sem.at[1])
    load_w = pltpu.make_async_copy(w_hbm, w_v, load_sem.at[2])
    load_s.start()
    load_x.start()
    load_w.start()

    barrier = pltpu.get_barrier_semaphore()
    partners = [y_peer, y_cross, sibling, x_peer] + z_to
    for partner in partners:
        pl.semaphore_signal(barrier, inc=1, device_id=partner, device_id_type=MESH)

    order = [k for k in range(1, deep)] + [0]
    span = WIDE * CORES * 2 * rows

    def turn(k):
        zz = lax.rem(z + k, deep)
        part = x_v[:, pl.ds(pl.multiple_of(zz * span, span), span)].T
        for xx in range(WIDE):
            for cy in range(CORES * 2):
                start = (xx * CORES * 2 + cy) * rows
                tx[k, cy, xx * rows:(xx + 1) * rows, :] = part[start:start + rows, :]

    load_x.wait()
    turn(order[0])
    load_s.wait()
    pl.semaphore_wait(barrier, len(partners))

    s_y = remote(s_v.at[me], s_v.at[me], s_send_sem.at[0], s_recv_sem.at[0], y_peer)
    s_sib = remote(s_v.at[me], s_v.at[me], s_send_sem.at[1], s_recv_sem.at[1], sibling)
    s_fwd = remote(s_v.at[from_y], s_v.at[from_y], s_send_sem.at[2], s_recv_sem.at[2], sibling)
    s_y.start()
    s_sib.start()

    x_copies = {}
    for n, k in enumerate(order):
        if n:
            turn(k)
        copies = []
        for slot, (device, there) in enumerate(
            ((y_peer, from_y), (y_cross, from_cross), (sibling, from_sib))
        ):
            copy = remote(
                tx.at[k, there], rx.at[k, me], x_send_sem.at[k, slot], x_recv_sem.at[k, slot], device
            )
            copy.start()
            copies.append(copy)
        x_copies[k] = copies
        rx[k, me] = tx[k, me]

    scales = []
    for cc in range(CORES):
        here = (z * WIDE + wide) * CORES + cc
        mine = list_ref[here]
        tally = jnp.int32(0)
        for h in range(groups):
            tally = tally + jnp.where(list_ref[h] == mine, mask_ref[h], 0)
        done = jnp.full((1, wg_ref.shape[1]), mask_ref[here], jnp.int32).astype(jnp.float32)
        total = jnp.full((1, wg_ref.shape[1]), tally, jnp.int32).astype(jnp.float32)
        scales.append(done / (total + 1.0 - done))

    load_w.wait()

    def grad(s_block):
        return lax.dot_general(
            s_block, w_v[...], (((1,), (1,)), ((), ())), preferred_element_type=jnp.float32
        ).astype(jnp.bfloat16)

    own_columns = pl.ds(pl.multiple_of(y * half, half), half)
    ig_ref[:, own_columns] = grad(s_v[me])

    s_y.wait_recv()
    s_fwd.start()
    ig_send[...] = grad(s_v[from_y])
    ig_copy = remote(ig_send, ig_ref.at[:, own_columns], ig_send_sem, ig_recv_sem, y_peer)
    ig_copy.start()

    s_sib.wait_recv()
    s_fwd.wait_recv()

    px_copies, z_copies = {}, {}

    def partial(k):
        for copy in x_copies[k]:
            copy.wait_recv()
        total = None
        for cc in range(CORES):
            left = jnp.concatenate([rx[k, cc * 2], rx[k, cc * 2 + 1]], axis=1)
            right = s_v[cc * 2:cc * 2 + 2].reshape(2 * tokens, s_v.shape[2])
            product = scales[cc] * jnp.dot(left, right, preferred_element_type=jnp.float32)
            total = product if total is None else total + product
        own_part[k, 0] = total[:rows]
        own_part[k, 1] = total[rows:]
        coded, scale = encode(own_part[k, 1 - wide])
        px_send[k] = coded
        px_scale[k] = scale

    def send_x(k):
        copies = [
            remote(px_send.at[k], px_recv.at[k], px_send_sem.at[k, 0], px_recv_sem.at[k, 0], x_peer),
            remote(px_scale.at[k], px_rscale.at[k], px_send_sem.at[k, 1], px_recv_sem.at[k, 1], x_peer),
        ]
        for copy in copies:
            copy.start()
        px_copies[k] = copies

    def gather_x(k):
        for copy in px_copies[k]:
            copy.wait_recv()
        value = own_part[k, wide] + decoded(px_recv[k], px_rscale[k])
        if k:
            coded, scale = encode(value)
            q_send[k] = coded
            q_scale[k] = scale
            copies = [
                remote(q_send.at[k], zr.at[k], z_send_sem.at[k, 0], z_recv_sem.at[k, 0], z_to[k - 1]),
                remote(q_scale.at[k], zr_scale.at[k], z_send_sem.at[k, 1], z_recv_sem.at[k, 1], z_to[k - 1]),
            ]
            for copy in copies:
                copy.start()
            z_copies[k] = copies
        else:
            q[...] = value

    for n, k in enumerate(order):
        partial(k)
        send_x(k)
        if n:
            gather_x(order[n - 1])
    gather_x(order[-1])

    total = q[...]
    for k in range(1, deep):
        for copy in z_copies[k]:
            copy.wait_recv()
        total = total + decoded(zr[k], zr_scale[k])
    wg_ref[...] = total

    ig_copy.wait_recv()

    for copy in (s_y, s_sib, s_fwd, ig_copy):
        copy.wait_send()
    for group in (x_copies, px_copies, z_copies):
        for copies in group.values():
            for copy in copies:
                copy.wait_send()


def kernel_shards(deep, rows, x, s, w, mask, plist):
    tokens, width = x.shape
    values = s.shape[1]
    f32, bf16, i16 = jnp.float32, jnp.bfloat16, jnp.int16
    dma = pltpu.SemaphoreType.DMA
    anywhere = pl.BlockSpec(memory_space=pl.ANY)
    smem = pl.BlockSpec(memory_space=pltpu.SMEM)
    wide_rows = WIDE * rows
    return pl.pallas_call(
        functools.partial(kernel, deep),
        out_shape=(
            pltpu.VMEM((tokens, width), bf16),
            pltpu.VMEM((rows, values), f32),
        ),
        in_specs=[smem, smem, anywhere, anywhere, anywhere],
        out_specs=(pl.BlockSpec(memory_space=pltpu.VMEM),) * 2,
        scratch_shapes=[
            pltpu.VMEM((tokens, width), bf16),
            pltpu.VMEM((CORES * 2, tokens, values), bf16),
            pltpu.VMEM(w.shape, bf16),
            pltpu.VMEM((deep, CORES * 2, wide_rows, tokens), bf16),
            pltpu.VMEM((deep, CORES * 2, wide_rows, tokens), bf16),
            pltpu.VMEM((deep, WIDE, rows, values), f32),
            pltpu.VMEM((deep, rows, values), i16),
            pltpu.VMEM((deep, 1, values), f32),
            pltpu.VMEM((deep, rows, values), i16),
            pltpu.VMEM((deep, 1, values), f32),
            pltpu.VMEM((rows, values), f32),
            pltpu.VMEM((deep, rows, values), i16),
            pltpu.VMEM((deep, 1, values), f32),
            pltpu.VMEM((deep, rows, values), i16),
            pltpu.VMEM((deep, 1, values), f32),
            pltpu.VMEM((tokens, w.shape[0]), bf16),
            dma((3,)), dma((3,)), dma((3,)), dma((deep, 3)), dma((deep, 3)),
            dma((deep, 2)), dma((deep, 2)), dma((deep, 2)), dma((deep, 2)), dma, dma,
        ],
        compiler_params=pltpu.CompilerParams(collective_id=0, has_side_effects=True),
    )(mask, plist, x, s, w)


def solution(mesh):
    outer, inner = mesh.shape["grp"], mesh.shape["fsdp"]

    def shards(x, s, w, mask, plist):
        rows = x.shape[1] // (outer * inner)
        if inner == 2 and outer % (CORES * WIDE) == 0 and rows % 16 == 0 and x.shape[0] % 128 == 0:
            return tuple(kernel_shards(outer // (CORES * WIDE), rows, x, s, w, mask, plist))
        return collective_shards(x, s, w, mask, plist)

    in_specs = (P(("grp", "fsdp"), None), P(("grp", "fsdp"), None), P("fsdp", None), P(), P())
    out_specs = (P(("grp", "fsdp"), None), P(("grp", "fsdp"), None))
    return jax.shard_map(shards, mesh=mesh, in_specs=in_specs, out_specs=out_specs, check_vma=False)
```

```python
import functools

import jax
import jax.numpy as jnp
from jax import lax
from jax.experimental import pallas as pl
from jax.experimental.pallas import tpu as pltpu
from jax.sharding import PartitionSpec as P

MESH = pl.DeviceIdType.MESH
CORES = 2
WIDE = 2
LAG = 2
STEPS = 32766.0
TINY = 1e-33


def collective_shards(
    normalized_inputs,
    output_sensitivity,
    projection_weights,
    completion_mask,
    replica_partition_list,
):
    replica_index = lax.axis_index("grp")
    selected_replica = lax.iota(jnp.int32, completion_mask.shape[0]) == replica_index
    assigned_piece = jnp.sum(jnp.where(selected_replica, replica_partition_list, 0))
    finished_indicator = jnp.sum(jnp.where(selected_replica, completion_mask, 0))
    finisher_tally = jnp.sum(
        jnp.where(replica_partition_list == assigned_piece, completion_mask, 0)
    )
    living_float = finished_indicator.astype(jnp.float32)
    decode_sum = living_float / (finisher_tally.astype(jnp.float32) + 1.0 - living_float)
    tokens_here = normalized_inputs.shape[0]
    model_width = normalized_inputs.shape[1]
    inner_size = lax.axis_size("fsdp")
    outer_size = lax.axis_size("grp")
    input_grad = lax.dot_general(
        output_sensitivity,
        lax.all_gather(projection_weights, "fsdp", axis=0, tiled=True),
        (((1,), (1,)), ((), ())),
        preferred_element_type=jnp.float32,
    ).astype(jnp.bfloat16)
    owner_rows = model_width // (outer_size * inner_size)
    reordered = normalized_inputs.reshape(tokens_here, outer_size, inner_size, owner_rows)
    reordered = reordered.transpose(0, 2, 1, 3).reshape(tokens_here, model_width)
    column_block = lax.all_to_all(reordered, "fsdp", split_axis=1, concat_axis=0, tiled=True)
    group_block = lax.dot_general(
        column_block,
        lax.all_gather(output_sensitivity, "fsdp", axis=0, tiled=True),
        (((0,), (0,)), ((), ())),
        preferred_element_type=jnp.float32,
    )
    weight_grad = lax.psum_scatter(decode_sum * group_block, "grp", scatter_dimension=0, tiled=True)
    return (input_grad, weight_grad)


def encode(value):
    top = jnp.maximum(jnp.max(jnp.abs(value), axis=0, keepdims=True), TINY)
    coded = jnp.round(value * (STEPS / top)).astype(jnp.int32).astype(jnp.int16)
    return coded, top * (1.0 / STEPS)


def decoded(coded, step):
    return coded.astype(jnp.int32).astype(jnp.float32) * step


def kernel(
    deep,
    mask_ref, list_ref, x_hbm, s_hbm, w_hbm,
    ig_ref, wg_ref,
    x_v, s_v, w_v, tx, rx, own_part, px_send, px_scale, px_recv, px_rscale,
    q, q_send, q_scale, zr, zr_scale, ig_send,
    load_sem, s_send_sem, s_recv_sem, x_send_sem, x_recv_sem,
    px_send_sem, px_recv_sem, z_send_sem, z_recv_sem, ig_send_sem, ig_recv_sem,
):
    grp = lax.axis_index("grp")
    y = lax.axis_index("fsdp")
    core = lax.rem(grp, CORES)
    wide = lax.rem(grp // CORES, WIDE)
    z = grp // (CORES * WIDE)
    oy, oc = 1 - y, 1 - core
    tokens = s_hbm.shape[0]
    groups = mask_ref.shape[0]
    rows = wg_ref.shape[0]
    half = w_hbm.shape[0]

    def at(zz, xx, cc, yy):
        return ((zz * WIDE + xx) * CORES + cc, yy)

    def remote(src, dst, send, recv, device):
        copy = pltpu.make_async_remote_copy(
            src_ref=src, dst_ref=dst, send_sem=send, recv_sem=recv,
            device_id=device, device_id_type=MESH,
        )
        return copy

    y_peer = at(z, wide, core, oy)
    y_cross = at(z, wide, oc, oy)
    sibling = at(z, wide, oc, y)
    x_peer = at(z, 1 - wide, core, y)
    z_to = [at(lax.rem(z + k, deep), wide, core, y) for k in range(1, deep)]
    me = core * 2 + y
    from_y = core * 2 + oy
    from_cross = oc * 2 + oy
    from_sib = oc * 2 + y

    load_s = pltpu.make_async_copy(s_hbm, s_v.at[me], load_sem.at[0])
    load_x = pltpu.make_async_copy(x_hbm, x_v, load_sem.at[1])
    load_w = pltpu.make_async_copy(w_hbm, w_v, load_sem.at[2])
    load_s.start()
    load_x.start()
    load_w.start()

    barrier = pltpu.get_barrier_semaphore()
    partners = [y_peer, y_cross, sibling, x_peer] + z_to
    for partner in partners:
        pl.semaphore_signal(barrier, inc=1, device_id=partner, device_id_type=MESH)

    order = [k for k in range(1, deep)] + [0]
    span = WIDE * CORES * 2 * rows

    def turn(k):
        zz = lax.rem(z + k, deep)
        part = x_v[:, pl.ds(pl.multiple_of(zz * span, span), span)].T
        for xx in range(WIDE):
            for cy in range(CORES * 2):
                start = (xx * CORES * 2 + cy) * rows
                tx[k, cy, xx * rows:(xx + 1) * rows, :] = part[start:start + rows, :]

    load_s.wait()
    pl.semaphore_wait(barrier, len(partners))

    s_y = remote(s_v.at[me], s_v.at[me], s_send_sem.at[0], s_recv_sem.at[0], y_peer)
    s_sib = remote(s_v.at[me], s_v.at[me], s_send_sem.at[1], s_recv_sem.at[1], sibling)
    s_fwd = remote(s_v.at[from_y], s_v.at[from_y], s_send_sem.at[2], s_recv_sem.at[2], sibling)
    s_y.start()
    s_sib.start()
    load_x.wait()

    x_copies = {}
    for n, k in enumerate(order):
        turn(k)
        copies = []
        for slot, (device, there) in enumerate(
            ((y_peer, from_y), (y_cross, from_cross), (sibling, from_sib))
        ):
            copy = remote(
                tx.at[k, there], rx.at[k, me], x_send_sem.at[k, slot], x_recv_sem.at[k, slot], device
            )
            copy.start()
            copies.append(copy)
        x_copies[k] = copies
        rx[k, me] = tx[k, me]

    scales = []
    for cc in range(CORES):
        here = (z * WIDE + wide) * CORES + cc
        mine = list_ref[here]
        tally = jnp.int32(0)
        for h in range(groups):
            tally = tally + jnp.where(list_ref[h] == mine, mask_ref[h], 0)
        done = jnp.full((1, wg_ref.shape[1]), mask_ref[here], jnp.int32).astype(jnp.float32)
        total = jnp.full((1, wg_ref.shape[1]), tally, jnp.int32).astype(jnp.float32)
        scales.append(done / (total + 1.0 - done))

    load_w.wait()

    def grad(s_block):
        return lax.dot_general(
            s_block, w_v[...], (((1,), (1,)), ((), ())), preferred_element_type=jnp.float32
        ).astype(jnp.bfloat16)

    own_columns = pl.ds(pl.multiple_of(y * half, half), half)
    ig_ref[:, own_columns] = grad(s_v[me])

    s_y.wait_recv()
    s_fwd.start()
    ig_send[...] = grad(s_v[from_y])
    ig_copy = remote(ig_send, ig_ref.at[:, own_columns], ig_send_sem, ig_recv_sem, y_peer)
    ig_copy.start()

    s_sib.wait_recv()
    s_fwd.wait_recv()

    px_copies, z_copies = {}, {}

    def partial(k):
        for copy in x_copies[k]:
            copy.wait_recv()
        total = None
        for cc in range(CORES):
            left = jnp.concatenate([rx[k, cc * 2], rx[k, cc * 2 + 1]], axis=1)
            right = s_v[cc * 2:cc * 2 + 2].reshape(2 * tokens, s_v.shape[2])
            product = scales[cc] * jnp.dot(left, right, preferred_element_type=jnp.float32)
            total = product if total is None else total + product
        own_part[k, 0] = total[:rows]
        own_part[k, 1] = total[rows:]
        coded, scale = encode(own_part[k, 1 - wide])
        px_send[k] = coded
        px_scale[k] = scale

    def send_x(k):
        copies = [
            remote(px_send.at[k], px_recv.at[k], px_send_sem.at[k, 0], px_recv_sem.at[k, 0], x_peer),
            remote(px_scale.at[k], px_rscale.at[k], px_send_sem.at[k, 1], px_recv_sem.at[k, 1], x_peer),
        ]
        for copy in copies:
            copy.start()
        px_copies[k] = copies

    def gather_x(k):
        for copy in px_copies[k]:
            copy.wait_recv()
        value = own_part[k, wide] + decoded(px_recv[k], px_rscale[k])
        if k:
            coded, scale = encode(value)
            q_send[k] = coded
            q_scale[k] = scale
            copies = [
                remote(q_send.at[k], zr.at[k], z_send_sem.at[k, 0], z_recv_sem.at[k, 0], z_to[k - 1]),
                remote(q_scale.at[k], zr_scale.at[k], z_send_sem.at[k, 1], z_recv_sem.at[k, 1], z_to[k - 1]),
            ]
            for copy in copies:
                copy.start()
            z_copies[k] = copies
        else:
            q[...] = value

    for n, k in enumerate(order):
        partial(k)
        send_x(k)
        if n >= LAG:
            gather_x(order[n - LAG])
    for k in order[max(deep - LAG, 0):]:
        gather_x(k)

    total = q[...]
    for k in range(1, deep):
        for copy in z_copies[k]:
            copy.wait_recv()
        total = total + decoded(zr[k], zr_scale[k])
    wg_ref[...] = total

    ig_copy.wait_recv()

    for copy in (s_y, s_sib, s_fwd, ig_copy):
        copy.wait_send()
    for group in (x_copies, px_copies, z_copies):
        for copies in group.values():
            for copy in copies:
                copy.wait_send()


def kernel_shards(deep, rows, x, s, w, mask, plist):
    tokens, width = x.shape
    values = s.shape[1]
    f32, bf16, i16 = jnp.float32, jnp.bfloat16, jnp.int16
    dma = pltpu.SemaphoreType.DMA
    anywhere = pl.BlockSpec(memory_space=pl.ANY)
    smem = pl.BlockSpec(memory_space=pltpu.SMEM)
    wide_rows = WIDE * rows
    return pl.pallas_call(
        functools.partial(kernel, deep),
        out_shape=(
            pltpu.VMEM((tokens, width), bf16),
            pltpu.VMEM((rows, values), f32),
        ),
        in_specs=[smem, smem, anywhere, anywhere, anywhere],
        out_specs=(pl.BlockSpec(memory_space=pltpu.VMEM),) * 2,
        scratch_shapes=[
            pltpu.VMEM((tokens, width), bf16),
            pltpu.VMEM((CORES * 2, tokens, values), bf16),
            pltpu.VMEM(w.shape, bf16),
            pltpu.VMEM((deep, CORES * 2, wide_rows, tokens), bf16),
            pltpu.VMEM((deep, CORES * 2, wide_rows, tokens), bf16),
            pltpu.VMEM((deep, WIDE, rows, values), f32),
            pltpu.VMEM((deep, rows, values), i16),
            pltpu.VMEM((deep, 1, values), f32),
            pltpu.VMEM((deep, rows, values), i16),
            pltpu.VMEM((deep, 1, values), f32),
            pltpu.VMEM((rows, values), f32),
            pltpu.VMEM((deep, rows, values), i16),
            pltpu.VMEM((deep, 1, values), f32),
            pltpu.VMEM((deep, rows, values), i16),
            pltpu.VMEM((deep, 1, values), f32),
            pltpu.VMEM((tokens, w.shape[0]), bf16),
            dma((3,)), dma((3,)), dma((3,)), dma((deep, 3)), dma((deep, 3)),
            dma((deep, 2)), dma((deep, 2)), dma((deep, 2)), dma((deep, 2)), dma, dma,
        ],
        compiler_params=pltpu.CompilerParams(collective_id=0, has_side_effects=True),
    )(mask, plist, x, s, w)


def solution(mesh):
    outer, inner = mesh.shape["grp"], mesh.shape["fsdp"]

    def shards(x, s, w, mask, plist):
        rows = x.shape[1] // (outer * inner)
        if inner == 2 and outer % (CORES * WIDE) == 0 and rows % 16 == 0 and x.shape[0] % 128 == 0:
            return tuple(kernel_shards(outer // (CORES * WIDE), rows, x, s, w, mask, plist))
        return collective_shards(x, s, w, mask, plist)

    in_specs = (P(("grp", "fsdp"), None), P(("grp", "fsdp"), None), P("fsdp", None), P(), P())
    out_specs = (P(("grp", "fsdp"), None), P(("grp", "fsdp"), None))
    return jax.shard_map(shards, mesh=mesh, in_specs=in_specs, out_specs=out_specs, check_vma=False)
```
